32 devices in a mesh: dp: 4 (over x, core), band: 8 (over z, y).
Axes of the slice: x: 2, y: 2, z: 4, core: 2. Of those that a mesh axis runs over, the one named last changes fastest.
Arguments:
- features: bfloat16 [8160, 256], P(('dp', 'band')), parts along dimension 0, may hold values from -6 to 6
- corners: int32 [8160, 512], P(('dp', 'band')), parts along dimension 0, may hold values from 0 to 1535, as said below
- bilinear: float32 [8160, 512], P(('dp', 'band')), parts along dimension 0, may hold values from 0.08 to 0.5, as said below
- attention: float32 [8160, 128], P(('dp', 'band')), parts along dimension 0, may hold values from 0 to 1, as said below
- w_value: bfloat16 [256, 256], replicated, may hold values from -0.375 to 0.375
- b_value: float32 [256], replicated, may hold values from -0.6 to 0.6
- w_out: bfloat16 [256, 256], replicated, may hold values from -1.5 to 1.5
- b_out: float32 [256], replicated, may hold values from -3 to 3
- norm1_gain: float32 [256], replicated, may hold values from 0.5 to 1.5
- norm1_bias: float32 [256], replicated, may hold values from -3 to 3
- w_in: bfloat16 [256, 1024], replicated, may hold values from -0.375 to 0.375
- b_in: float32 [1024], replicated, may hold values from -3 to 3
- w_ffout: bfloat16 [1024, 256], replicated, may hold values from -0.1875 to 0.1875
- b_ffout: float32 [256], replicated, may hold values from -3 to 3
- norm2_gain: float32 [256], replicated, may hold values from 0.5 to 1.5
- norm2_bias: float32 [256], replicated, may hold values from -3 to 3
Outputs:
- encoded: bfloat16 [8160, 256], P(('dp', 'band')), parts along dimension 0
The draws below stay inside these ranges and needn't reach their ends.
There are 4 independent parts, one for each index of `dp`. The reference program is written for one: setup_inputs(seed, part) draws one part's arguments, and reference() takes and returns one part's arrays. A program takes and returns all parts, laid end to end along the dimension named above; an argument that names none is the same for every part. Nothing has to cross between parts.
Inputs may be any that keep to these rules, and one draw needn't show every extreme that they name: An entry for level l is a row of a map of 192 * 8 // 4**l tokens laid out in rows of 128 // 2**l; the four corners of a point are k, k + 1, k + 128 // 2**l and k + 128 // 2**l + 1 in that order. `bilinear`: the four corner weights of a point are positive and sum to one. `attention`: for each token and head the 16 weights are positive and sum to one.
All inputs are finite; a program needn't handle non-finite values.
Results may differ from the reference program's by a relative error of at most 0.009.
Values may be sent and summed in bfloat16 or wider, within the bound.
No kernel may reach another device: no remote copies, remote signals or barrier semaphores. Data moves between devices by JAX's collectives and lax.ppermute only.
A program may use at most 64 MiB of HBM per device.

```python
import jax
import jax.numpy as jnp
from jax import lax

D = 256
HEADS = 8
FF = 1024
LEVELS = 4
POINTS = 4
MAP_W = 128
ROWS_DEV = 192
BAND_ROWS = 255
TOKENS = 2040


def query_place():
    band_total = TOKENS // BAND_ROWS
    token_ids = jnp.arange(TOKENS, dtype=jnp.int32)
    band_index = token_ids // BAND_ROWS
    local_row = token_ids % BAND_ROWS
    own_position = band_index * ROWS_DEV + local_row
    own_length = jnp.zeros((TOKENS,), jnp.int32) + ROWS_DEV * band_total
    offset_rows = 0
    for level_index in range(LEVELS):
        rows_here = ROWS_DEV // 4 ** level_index
        inside = (local_row >= offset_rows) & (local_row < offset_rows + rows_here)
        own_position = jnp.where(inside, band_index * rows_here + local_row - offset_rows, own_position)
        own_length = jnp.where(inside, rows_here * band_total, own_length)
        offset_rows = offset_rows + rows_here
    return (own_position, own_length)


def draw_corners(key, part):
    band_total = TOKENS // BAND_ROWS
    own_position, own_length = query_place()
    tables = []
    for level_index in range(LEVELS):
        rows_here = ROWS_DEV // 4 ** level_index
        length = rows_here * band_total
        stride = MAP_W // 2 ** level_index
        shape_here = (TOKENS, HEADS, POINTS)
        keys_here = jax.random.split(jax.random.fold_in(key, 11 + level_index), 4)
        centre = (own_position * length // own_length)[:, None, None]
        jitter = jax.random.randint(keys_here[0], shape_here, -rows_here, rows_here + 1) + jax.random.randint(keys_here[1], shape_here, -rows_here, rows_here + 1)
        faraway = jax.random.randint(keys_here[2], shape_here, 0, length)
        choose = jax.random.randint(keys_here[3], shape_here, 0, 4) != 0
        anchor = jnp.clip(jnp.where(choose, faraway, centre + jitter), 0, length - stride - 2)
        tables.append(jnp.stack([anchor, anchor + 1, anchor + stride, anchor + stride + 1], axis=-1))
    return jnp.stack(tables, axis=2).reshape(TOKENS, HEADS * LEVELS * POINTS * 4).astype(jnp.int32)


def draw_bilinear(key, part):
    key_first, key_second = jax.random.split(jax.random.fold_in(key, 29))
    shape_here = (TOKENS, HEADS * LEVELS * POINTS)
    first = jax.random.uniform(key_first, shape_here, jnp.float32)
    second = jax.random.uniform(key_second, shape_here, jnp.float32)
    first = 0.3 + 0.4 * first
    second = 0.3 + 0.4 * second
    stacked = jnp.stack([(1.0 - first) * (1.0 - second), first * (1.0 - second), (1.0 - first) * second, first * second], axis=-1)
    return stacked.reshape(TOKENS, HEADS * LEVELS * POINTS * 4).astype(jnp.float32)


def draw_attention(key, part):
    key_logit = jax.random.fold_in(key, 37)
    shape_here = (TOKENS, HEADS, LEVELS * POINTS)
    finer = jnp.arange(LEVELS * POINTS, dtype=jnp.int32) // POINTS < 2
    noise = jax.random.normal(key_logit, shape_here, jnp.float32)
    logits = jnp.where(finer, 0.3 * noise, 1.35 + 0.8 * noise)
    return jax.nn.softmax(logits, axis=-1).reshape(TOKENS, HEADS * LEVELS * POINTS).astype(jnp.float32)


def block_scale(stream_key, shape, pieces, smallest, top_value):
    def one(axis_at, shards_of):
        steps = jax.random.uniform(jax.random.fold_in(jax.random.fold_in(stream_key, 6), axis_at), (shards_of,), jnp.float32, smallest / len(pieces), top_value / len(pieces))
        return jnp.repeat(jnp.exp(steps), shape[axis_at] // shards_of).reshape((-1,) + (1,) * (len(shape) - axis_at - 1))

    level = one(*pieces[0])
    for cut in pieces[1:]:
        level = level * one(*cut)
    return level


def bell_draw(rng, dims, deviation, limit, pieces=(), held_as=jnp.bfloat16):
    loudness = block_scale(rng, dims, pieces, -0.22, 0.18) if pieces else 1.0
    values = jax.random.normal(rng, dims, jnp.float32) * deviation * loudness
    return jnp.minimum(jnp.maximum(values, -limit), limit).astype(held_as)


def setup_inputs(seed: int = 0, part: int = 0) -> dict:
    key_list = jax.random.split(jax.random.key(seed), 17)
    own_keys = jax.random.split(jax.random.fold_in(key_list[16], part), 17)
    return {
        "features": bell_draw(own_keys[0], (TOKENS, D), 1.0, 6.0, ((0, 8),)),
        "corners": draw_corners(jax.random.fold_in(jax.random.fold_in(key_list[16], part), 71), part),
        "bilinear": draw_bilinear(jax.random.fold_in(jax.random.fold_in(key_list[16], part), 71), part),
        "attention": draw_attention(jax.random.fold_in(jax.random.fold_in(key_list[16], part), 71), part),
        "w_value": bell_draw(key_list[4], (D, D), D ** -0.5, 0.375),
        "b_value": bell_draw(key_list[5], (D,), 0.1, 0.6, (), jnp.float32),
        "w_out": bell_draw(key_list[6], (D, D), (D // 16) ** -0.5, 1.5),
        "b_out": bell_draw(key_list[7], (D,), 0.5, 3.0, (), jnp.float32),
        "norm1_gain": jnp.clip(1.0 + 0.1 * jax.random.normal(key_list[8], (D,), jnp.float32), 0.5, 1.5),
        "norm1_bias": bell_draw(key_list[9], (D,), 0.5, 3.0, (), jnp.float32),
        "w_in": bell_draw(key_list[10], (D, FF), D ** -0.5, 0.375),
        "b_in": bell_draw(key_list[11], (FF,), 0.5, 3.0, (), jnp.float32),
        "w_ffout": bell_draw(key_list[12], (FF, D), FF ** -0.5, 0.1875),
        "b_ffout": bell_draw(key_list[13], (D,), 0.5, 3.0, (), jnp.float32),
        "norm2_gain": jnp.clip(1.0 + 0.1 * jax.random.normal(key_list[14], (D,), jnp.float32), 0.5, 1.5),
        "norm2_bias": bell_draw(key_list[15], (D,), 0.5, 3.0, (), jnp.float32),
    }


def layer_norm(inputs, gain, shift):
    average = lax.optimization_barrier(jnp.mean(inputs, axis=-1, keepdims=True))
    centred = inputs - average
    variance = lax.optimization_barrier(jnp.mean(centred * centred, axis=-1, keepdims=True))
    return centred * lax.rsqrt(variance + 1e-05) * gain + shift

def reference(features, corners, bilinear, attention, w_value, b_value, w_out, b_out, norm1_gain, norm1_bias, w_in, b_in, w_ffout, b_ffout, norm2_gain, norm2_bias):
    token_count, model_width = features.shape
    head_dim = model_width // HEADS
    samples = LEVELS * POINTS * 4
    segment_rows = [ROWS_DEV // 4 ** level_index for level_index in range(LEVELS)]
    segment_start = [sum(segment_rows[:level_index]) for level_index in range(LEVELS)]
    value_rows = (jnp.dot(features, w_value, preferred_element_type=jnp.float32) + b_value).astype(jnp.bfloat16)
    weight = (attention.reshape(token_count, HEADS, LEVELS, POINTS, 1) * bilinear.reshape(token_count, HEADS, LEVELS, POINTS, 4)).astype(jnp.bfloat16)
    weight = weight.reshape(token_count, HEADS, samples)
    corner_table = corners.reshape(token_count, HEADS, LEVELS, POINTS * 4)
    places = []
    for level_index in range(LEVELS):
        level_corner = corner_table[:, :, level_index]
        places.append(level_corner // segment_rows[level_index] * BAND_ROWS + segment_start[level_index] + level_corner % segment_rows[level_index])
    place_table = jnp.stack(places, axis=2).reshape(token_count, HEADS, samples)
    flat_index = (place_table * HEADS + jnp.arange(HEADS, dtype=jnp.int32)[None, :, None]).astype(jnp.int32)
    flat_value = value_rows.reshape(token_count * HEADS, head_dim)
    band_count = token_count // BAND_ROWS

    def blend_block(block_args):
        index_block, weight_block = block_args
        picked = flat_value[index_block].astype(jnp.float32)
        return lax.optimization_barrier(jnp.sum(weight_block.astype(jnp.float32)[..., None] * picked, axis=2))
    sampled = lax.map(blend_block, (flat_index.reshape(band_count, BAND_ROWS, HEADS, samples), weight.reshape(band_count, BAND_ROWS, HEADS, samples)))
    sampled = sampled.reshape(token_count, model_width).astype(jnp.bfloat16)
    attended = jnp.dot(sampled, w_out, preferred_element_type=jnp.float32) + b_out
    middle = layer_norm(features.astype(jnp.float32) + attended, norm1_gain, norm1_bias).astype(jnp.bfloat16)
    hidden = jnp.maximum(jnp.dot(middle, w_in, preferred_element_type=jnp.float32) + b_in, 0.0).astype(jnp.bfloat16)
    result = middle.astype(jnp.float32) + jnp.dot(hidden, w_ffout, preferred_element_type=jnp.float32) + b_ffout
    return layer_norm(result, norm2_gain, norm2_bias).astype(jnp.bfloat16)
```

```python
import functools

import jax
import jax.numpy as jnp
from jax import lax
from jax.experimental import pallas as pl
from jax.experimental.pallas import tpu as pltpu
from jax.sharding import PartitionSpec as P

HEADS = 8
LEVELS = 4
POINTS = 4
ROWS_DEV = 192
MAP_W = 128
BF = jnp.bfloat16
F32 = jnp.float32
GRAN = 16
MIB = 2**20


def table_kernel(n, heads_here, part, corners_ref, bilinear_ref, attention_ref, table_ref, pad_ref, k_ref, w_ref, a_ref):
    rows = corners_ref.shape[0]
    cols = corners_ref.shape[1]
    pts = cols // 4
    q = pad_ref.shape[0]
    def flip(x):
        pad_ref[0:rows, :] = x
        return pad_ref[...].T
    pad_ref[rows-7:q, :] = jnp.zeros((q-rows+7, 128), F32)
    att_t = flip(attention_ref[...])
    per = 128 // (128 // pts)
    att_t = att_t[part*pts:(part+1)*pts]
    for piece in range(cols // 128):
        sl = slice(piece*128, piece*128+128)
        k_ref[2*piece:2*piece+2] = flip(corners_ref[:, sl].astype(F32)).reshape(2, 64, q)
        w_ref[2*piece:2*piece+2] = flip(bilinear_ref[:, sl]).reshape(2, 64, q)
    a_ref[...] = att_t.reshape(heads_here, 16, q)
    lanes = 128
    sub = lax.broadcasted_iota(jnp.int32, (GRAN, lanes), 0).astype(F32)
    zero = jnp.zeros((GRAN, lanes), BF)
    def spread(row):
        return jnp.broadcast_to(row, (GRAN, lanes)).astype(BF)
    def head_body(hh, _):
        for qt in range(q // lanes):
            ql = slice(qt*lanes, (qt+1)*lanes)
            def krow(l, p):
                return k_ref[hh, l*16+p*4:l*16+p*4+1, ql]
            def wfull(l, p, c):
                return jnp.broadcast_to(w_ref[hh, l*16+p*4+c:l*16+p*4+c+1, ql], (GRAN, lanes))
            def afull(l, p):
                return jnp.broadcast_to(a_ref[hh, l*4+p:l*4+p+1, ql], (GRAN, lanes))
            row_base = 0
            for l in range(2):
                width = MAP_W >> l
                seg = ROWS_DEV // 4**l
                total = seg * n
                map_rows = total // width
                xs=[]; ys=[]; ws=[]
                for p in range(POINTS):
                    k = krow(l, p)
                    y = jnp.floor(k * (1.0/width))
                    xs.append(spread(k - y*width)); ys.append(spread(y))
                    a=afull(l,p); ws.append([(wfull(l,p,c)*a).astype(BF) for c in range(4)])
                for xg in range(width // GRAN):
                    here = (sub + float(xg*GRAN)).astype(BF)
                    before = (sub + float(xg*GRAN-1)).astype(BF)
                    tops=[]; bots=[]; extra=[]
                    for p in range(POINTS):
                        m0 = xs[p] == here
                        m1 = xs[p] == before
                        w0,w1,w2,w3 = ws[p]
                        tops.append(jnp.where(m0, w0, jnp.where(m1, w1, zero)))
                        if xg == 0:
                            mw = (xs[p] - here) == jnp.asarray(width-1, BF)
                            mw = mw & (here == jnp.zeros((), BF))
                            bots.append(jnp.where(m0, w2, jnp.where(m1, w3, jnp.where(mw, w1, zero))))
                            extra.append(jnp.where(mw, w3, zero))
                        else:
                            bots.append(jnp.where(m0, w2, jnp.where(m1, w3, zero)))
                    hit1=[None]*POINTS; hit2=[None]*POINTS
                    for y in range(map_rows):
                        acc=None
                        for p in range(POINTS):
                            hit = ys[p] == jnp.asarray(y, BF)
                            v = zero
                            if xg == 0 and y >= 2:
                                v = jnp.where(hit2[p], extra[p], v)
                            if y >= 1:
                                v = jnp.where(hit1[p], bots[p], v)
                            v = jnp.where(hit, tops[p], v)
                            acc = v if acc is None else acc + v
                            hit2[p]=hit1[p]; hit1[p]=hit
                        g = y*(width//GRAN)+xg
                        b = g // (seg//GRAN); r = row_base + GRAN*(g % (seg//GRAN))
                        table_ref[hh, b, r:r+GRAN, ql] = acc
                row_base += seg
            seg2 = ROWS_DEV//16; seg3 = ROWS_DEV//64
            w2_, w3_ = MAP_W>>2, MAP_W>>3
            mid = seg2*n//2
            low = sub < float(seg2)
            pos=[]; wts=[]
            for p in range(POINTS):
                k2 = jnp.broadcast_to(krow(2,p), (GRAN,lanes)); k3 = jnp.broadcast_to(krow(3,p), (GRAN,lanes))
                a=jnp.where(low, afull(2,p), afull(3,p))
                wc=[(jnp.where(low, wfull(2,p,c), wfull(3,p,c))*a).astype(BF) for c in range(4)]
                pos.append([jnp.where(low, k2 + float(o2-mid), k3 + float(o3-mid)).astype(BF) for o2,o3 in ((0,0),(1,1),(w2_,w3_),(w2_+1,w3_+1))])
                wts.append(wc)
            for b in range(n):
                tgt = jnp.where(low, sub + float(seg2*b - mid), jnp.where(sub < float(seg2+seg3), sub + float(seg3*b - seg2 - mid), -512.0)).astype(BF)
                acc=None
                for p in range(POINTS):
                    v=zero
                    for c in range(4):
                        v=jnp.where(pos[p][c]==tgt, wts[p][c], v)
                    acc = v if acc is None else acc+v
                table_ref[hh, b, row_base:row_base+GRAN, ql] = acc
        return 0
    lax.fori_loop(0, heads_here, head_body, 0)


def cost(us):
    return pl.CostEstimate(flops=int(us * 2.0e8), bytes_accessed=1000, transcendentals=0)


def build_tables(n, corners, bilinear, attention, part, heads_here):
    rows = corners.shape[0]
    q = -(-rows // 128) * 128
    cols = heads_here * 64
    return pl.pallas_call(
        functools.partial(table_kernel, n, heads_here, part),
        grid=(1,),
        in_specs=[
            pl.BlockSpec((rows, cols), lambda i: (0, part)),
            pl.BlockSpec((rows, cols), lambda i: (0, part)),
            pl.BlockSpec((rows, 128), lambda i: (0, 0)),
        ],
        out_specs=pl.BlockSpec((heads_here, n, 256, q), lambda i: (0, 0, 0, 0)),
        out_shape=jax.ShapeDtypeStruct((heads_here, n, 256, q), BF),
        scratch_shapes=[
            pltpu.VMEM((q, 128), F32),
            pltpu.VMEM((heads_here, 64, q), F32),
            pltpu.VMEM((heads_here, 64, q), F32),
            pltpu.VMEM((heads_here, 16, q), F32),
        ],
        compiler_params=pltpu.CompilerParams(vmem_limit_bytes=16 * MIB),
        cost_estimate=cost(3.0),
        name="tables",
    )(corners, bilinear, attention)


def prepare_kernel(wv, wo, wi, wf, b1, b2, b3, b4, b5, b6, b7, b8, feat, wv_t, wo_t, wi_t, wf_t, cols_t, bin_t, feat_t, pad):
    wv_t[...] = wv[...].astype(F32).T.astype(BF)
    wo_t[...] = wo[...].astype(F32).T.astype(BF)
    wi_t[...] = wi[...].astype(F32).T.astype(BF)
    wf_t[...] = wf[...].astype(F32).T.astype(BF)
    for i, b in enumerate((b1, b2, b3, b4, b5, b6, b7)):
        cols_t[i] = jnp.broadcast_to(b[...], (128, b.shape[1])).T
    bin_t[...] = jnp.broadcast_to(b8[...], (128, b8.shape[1])).T
    rows = feat.shape[0]
    q = pad.shape[0]
    pad[q - 8 : q] = jnp.zeros((8, pad.shape[1]), F32)
    pad[0:rows] = feat[...].astype(F32)
    feat_t[...] = pad[...].T


def prepare(wv, wo, wi, wf, biases, b_in, feat):
    d = wv.shape[0]
    ff = wi.shape[1]
    q = -(-feat.shape[0] // 128) * 128
    return pl.pallas_call(
        prepare_kernel,
        out_shape=(
            jax.ShapeDtypeStruct((d, d), BF),
            jax.ShapeDtypeStruct((d, d), BF),
            jax.ShapeDtypeStruct((ff, d), BF),
            jax.ShapeDtypeStruct((d, ff), BF),
            jax.ShapeDtypeStruct((7, d, 128), F32),
            jax.ShapeDtypeStruct((ff, 128), F32),
            jax.ShapeDtypeStruct((d, q), F32),
        ),
        scratch_shapes=[pltpu.VMEM((q, d), F32)],
        compiler_params=pltpu.CompilerParams(vmem_limit_bytes=16 * MIB),
        cost_estimate=cost(1.5),
        name="prepare",
    )(wv, wo, wi, wf, *[b.reshape(1, -1) for b in biases], b_in.reshape(1, -1), feat)


def wide(column, q):
    return jnp.concatenate([column] * (q // 128), axis=1)


def apply_block(block, band, wv_t, bias_v, tables, acc, blk):
    rows = block.shape[0]
    q = acc.shape[1]
    blk[0:rows] = block[...]
    value = lax.dot_general(
        wv_t[...], blk[...], (((1,), (1,)), ((), ())), preferred_element_type=F32
    )
    value = (value + wide(bias_v, value.shape[1])).astype(BF)
    dim = value.shape[0] // HEADS
    h = 0
    for table in tables:
        for j in range(table.shape[0]):
            rows_h = slice(h * dim, (h + 1) * dim)
            acc[rows_h] += jnp.dot(value[rows_h], table[j, band], preferred_element_type=F32)
            h += 1


def clear_tail(blk, rows):
    blk[rows - rows % 16 :] = jnp.zeros((blk.shape[0] - rows + rows % 16, blk.shape[1]), BF)


def mix_kernel(count, parts, first, *refs):
    bands = refs[0]
    blocks = refs[1 : 1 + count]
    wv_t, cols_t = refs[1 + count : 3 + count]
    tables = refs[3 + count : 3 + count + parts]
    at = 3 + count + parts
    acc_in = None if first else refs[at]
    acc, blk = refs[-2:]
    acc[...] = jnp.zeros_like(acc) if first else acc_in[...]
    clear_tail(blk, blocks[0].shape[0])
    bias_v = cols_t[0]
    for i in range(count):
        apply_block(blocks[i], bands[i], wv_t, bias_v, tables, acc, blk)


VM = pl.BlockSpec(memory_space=pltpu.VMEM)
SM = pl.BlockSpec(memory_space=pltpu.SMEM)


def mix(bands, blocks, wv_t, cols_t, tables, acc):
    d = wv_t.shape[0]
    q = tables[0].shape[-1]
    first = acc is None
    args = [bands, *blocks, wv_t, cols_t, *tables] + ([] if first else [acc])
    return pl.pallas_call(
        functools.partial(mix_kernel, len(blocks), len(tables), first),
        in_specs=[SM] + [VM] * (len(args) - 1),
        out_specs=VM,
        out_shape=jax.ShapeDtypeStruct((d, q), F32),
        scratch_shapes=[pltpu.VMEM((256, d), BF)],
        compiler_params=pltpu.CompilerParams(vmem_limit_bytes=16 * MIB),
        cost_estimate=cost(0.5 * len(blocks)),
        name="mix",
    )(*args)


def norm_t(x, gain, shift):
    inv = 1.0 / x.shape[0]
    centred = x - jnp.sum(x, axis=0, keepdims=True) * inv
    variance = jnp.sum(centred * centred, axis=0, keepdims=True) * inv
    return centred * lax.rsqrt(variance + 1e-05) * gain + shift


def tail_kernel(count, parts, *refs):
    bands = refs[0]
    blocks = refs[1 : 1 + count]
    wv_t, cols_t = refs[1 + count : 3 + count]
    tables = refs[3 + count : 3 + count + parts]
    acc_in, wo_t, wi_t, wf_t, bin_t, feat_t, out, acc, blk = refs[3 + count + parts :]
    q = acc.shape[1]
    acc[...] = acc_in[...]
    clear_tail(blk, blocks[0].shape[0])
    for i in range(count):
        apply_block(blocks[i], bands[i], wv_t, cols_t[0], tables, acc, blk)
    sampled = acc[...].astype(BF)
    attended = jnp.dot(wo_t[...], sampled, preferred_element_type=F32) + wide(cols_t[1], q)
    middle = norm_t(feat_t[...] + attended, wide(cols_t[2], q), wide(cols_t[3], q)).astype(BF)
    hidden = jnp.dot(wi_t[...], middle, preferred_element_type=F32) + wide(bin_t[...], q)
    hidden = jnp.maximum(hidden, 0.0).astype(BF)
    result = middle.astype(F32) + jnp.dot(wf_t[...], hidden, preferred_element_type=F32) + wide(cols_t[4], q)
    encoded = norm_t(result, wide(cols_t[5], q), wide(cols_t[6], q))
    out[...] = encoded.T.astype(BF)[0 : out.shape[0]]


def tail(bands, blocks, wv_t, cols_t, tables, acc, wo_t, wi_t, wf_t, bin_t, feat_t):
    d = wv_t.shape[0]
    q = tables[0].shape[-1]
    args = [bands, *blocks, wv_t, cols_t, *tables, acc, wo_t, wi_t, wf_t, bin_t, feat_t]
    return pl.pallas_call(
        functools.partial(tail_kernel, len(blocks), len(tables)),
        in_specs=[SM] + [VM] * (len(args) - 1),
        out_specs=VM,
        out_shape=jax.ShapeDtypeStruct((blocks[0].shape[0], d), BF),
        scratch_shapes=[pltpu.VMEM((d, q), F32), pltpu.VMEM((256, d), BF)],
        compiler_params=pltpu.CompilerParams(vmem_limit_bytes=16 * MIB),
        cost_estimate=cost(2.5),
        name="tail",
    )(*args)


def body(n, features, corners, bilinear, attention, w_value, b_value, w_out, b_out,
         norm1_gain, norm1_bias, w_in, b_in, w_ffout, b_ffout, norm2_gain, norm2_bias):
    half = n // 2
    ring = [2 * i for i in range(half)] + [2 * (n - 1 - i) + 1 for i in range(half, n)]
    up = [(ring[i], ring[(i + 1) % n]) for i in range(n)]
    down = [(b, a) for a, b in up]
    me = lax.axis_index("band")
    place = jnp.where(me % 2 == 0, me // 2, n - 1 - me // 2)

    def band_at(step):
        spot = (place + step) % n
        return jnp.where(spot < half, 2 * spot, 2 * (n - 1 - spot) + 1).astype(jnp.int32)

    prep = prepare(
        w_value, w_out, w_in, w_ffout,
        (b_value, b_out, norm1_gain, norm1_bias, b_ffout, norm2_gain, norm2_bias), b_in, features,
    )
    wv_t, wo_t, wi_t, wf_t, cols_t, bin_t, feat_t = prep
    tables = [build_tables(n, corners, bilinear, attention, part, 2) for part in range(HEADS // 2)]
    blocks = [(features, 0)]
    right = left = features
    for step in range(1, half):
        right = lax.ppermute(right, "band", up)
        left = lax.ppermute(left, "band", down)
        blocks += [(right, -step), (left, step)]
    last = lax.ppermute(right, "band", up)

    def gather(group):
        return jnp.stack([band_at(s) for _, s in group]), [b for b, _ in group]

    acc = None
    done = 0
    for size in [3] + [2] * n:
        group = blocks[done : done + size]
        if not group:
            break
        ids, arrays = gather(group)
        acc = mix(ids, arrays, wv_t, cols_t, tables, acc)
        done += size
    ids, arrays = gather([(last, -half)])
    return tail(ids, arrays, wv_t, cols_t, tables, acc, wo_t, wi_t, wf_t, bin_t, feat_t)


def solution(mesh):
    n = mesh.shape["band"]
    rows = P(("dp", "band"), None)
    in_specs = (rows,) * 4 + (P(),) * 12
    return jax.shard_map(
        functools.partial(body, n), mesh=mesh, in_specs=in_specs, out_specs=rows, check_vma=False
    )
```
